32 devices in a mesh: expert: 4 (over z), shard: 8 (over y, x, core).
Axes of the slice: x: 2, y: 2, z: 4, core: 2. Of those that a mesh axis runs over, the one named last changes fastest.
Arguments:
- tokens: bfloat16 [96, 6144], P('expert', 'shard'), may hold values from -6 to 6
- routes: int32 [96, 2], P('expert'), may hold values from 0 to 7, all different within a row; in each aligned block of 24 rows (0 to 23, 24 to 47, ...) at most 12 rows name the same one
- w_router: bfloat16 [6144, 8], replicated, may hold values from -0.078125 to 0.078125
- w_gate: bfloat16 [6144, 65536], P(None, ('expert', 'shard')), may hold values from -0.078125 to 0.078125
- w_up: bfloat16 [6144, 65536], P(None, ('expert', 'shard')), may hold values from -0.078125 to 0.078125
- w_down: bfloat16 [65536, 6144], P(('expert', 'shard')), may hold values from -0.125 to 0.125
Outputs:
- mixed: bfloat16 [96, 6144], P('expert', 'shard')
The draws below stay inside these ranges and needn't reach their ends.
Inputs may be any that keep to these rules, and one draw needn't show every extreme that they name: `routes`: the two experts of a row differ; within each aligned block of 24 rows no expert is named more than 24 / 2 times, and some expert is named exactly that often.
All inputs are finite; a program needn't handle non-finite values.
Results may differ from the reference program's by a relative error of at most 0.017.
Values may be sent and summed in bfloat16 or wider, within the bound.
A program may use at most 256 MiB of HBM per device.

```python
import math
import jax
import jax.numpy as jnp
import numpy as np
from jax import lax

D = 6144
EXPERTS = 8
FF_W = 8192
TOK_DEV = 24
TOKENS = 96
N_EXPERT = 4
N_SHARD = 8


def strengthened(drawn, stream_key, source, target, blocks, factor):
    def block_of(dim):
        return (jnp.arange(drawn.shape[dim]) // (drawn.shape[dim] // blocks)).reshape((-1,) + (1,) * (drawn.ndim - 1 - dim))

    first = jax.random.permutation(stream_key, blocks)[block_of(target)]
    second = (block_of(target) + blocks // 2) % blocks
    return jnp.where((block_of(source) == first) | (block_of(source) == second), factor * drawn, drawn)


def block_scale(own_key, dims, shards, low, high):
    loudness, own = 1.0, jax.random.fold_in(own_key, 6)
    for dim, shards_of in shards:
        draws = jnp.exp(jax.random.uniform(jax.random.fold_in(own, dim), (shards_of,), jnp.float32, low / len(shards), high / len(shards)))
        loudness = loudness * jnp.repeat(draws, dims[dim] // shards_of).reshape([-1 if axis == dim else 1 for axis in range(len(dims))])
    return loudness


def assign_block(rng, own, number, rows, number_of, top, bound, lean):
    sequence = jax.random.permutation(rng, number_of)
    heavy_load, usual = shares(number_of, rows * top, bound, lean, True), shares(number_of, rows * top, bound, lean, False)
    places = jnp.arange(number_of)

    def named(sizes, offset_by):
        used = int((sizes > 0).sum())
        fixed = max(1, used // 4)
        moved = fixed + (places - fixed + offset_by * (used - fixed)) % max(1, number_of - fixed)
        return jnp.zeros((number_of,), jnp.int32).at[sequence[jnp.where(places < fixed, places, moved)]].set(jnp.asarray(sizes, jnp.int32))

    sizes = jnp.where(number % 4 == 0, named(heavy_load, number // 4), named(usual, number - number // 4 - 1))
    mixed = jax.random.permutation(jax.random.fold_in(own, 3), number_of)
    source_of, sink = mixed[0:number_of // 2 * 2:2], mixed[1:number_of // 2 * 2:2]
    margin = jnp.minimum(sizes[source_of] - 1, bound - sizes[sink]) // 2
    margin = jnp.where((source_of == sequence[0]) | (sink == sequence[0]) | (sizes[sink] == 0), 0, jnp.maximum(margin, 0))
    moved = jax.random.randint(jax.random.fold_in(own, 4), (number_of // 2,), 0, 1 << 20) % (margin + 1)
    sizes = sizes.at[source_of].add(-moved).at[sink].add(moved)
    items = jnp.searchsorted(jnp.cumsum(sizes), jnp.arange(rows * top), side="right").astype(jnp.int32)
    table = items.reshape(top, rows).T
    table = table[jax.random.permutation(jax.random.fold_in(own, 1), rows)]
    offset_by = jax.random.randint(jax.random.fold_in(own, 2), (rows, 1), 0, top)
    return jnp.take_along_axis(table, (jnp.arange(top)[None, :] + offset_by) % top, axis=1)


def shares(number_of, total, most, skew, full):
    portions = [(1 << 20) // math.isqrt(rank ** skew) + 1 for rank in range(1, number_of + 1)]
    largest = most if full else min(most, max(-(-total // number_of), total * portions[0] // sum(portions)))
    least = 1 if total - largest >= number_of - 1 else 0
    counts, surplus = [largest] + [least] * (number_of - 1), total - largest - least * (number_of - 1)
    while surplus > 0:
        free = [i for i in range(1, number_of) if counts[i] < largest] or [i for i in range(1, number_of) if counts[i] < most]
        whole, left = sum([portions[i] for i in free]), surplus
        for i in free:
            addition = min(most - counts[i], max(1, left * portions[i] // whole), surplus)
            counts[i] = counts[i] + addition
            surplus = surplus - addition
    return np.array(counts)


def gaussian(rng, extent, scale, bound, split=(), held_as=jnp.bfloat16):
    drawn = jax.random.normal(rng, extent, jnp.float32) * scale
    if len(split) > 0:
        drawn = block_scale(rng, extent, split, -0.22, 0.18) * drawn
    return jnp.clip(drawn, min=-bound, max=bound).astype(held_as)


def heavy_noise(own_key, dims, spread, limit, split, heavy, held_as=jnp.bfloat16):
    entries = spread * jax.random.normal(own_key, dims, jnp.float32)
    if split:
        entries = entries * block_scale(own_key, dims, split, -0.22, 0.18)
    return jnp.clip(strengthened(entries, jax.random.fold_in(own_key, 3), *heavy), -limit, limit).astype(held_as)


def setup_inputs(seed: int = 0) -> dict:
    arg_keys = jax.random.split(jax.random.key(seed), 7)
    tokens = gaussian(arg_keys[0], (TOKENS, D), 1.0, 6.0, ((0, 4), (1, 8)))
    routes_keys = jax.random.split(jax.random.fold_in(arg_keys[1], 1), TOKENS // TOK_DEV)
    routes_turns = jax.random.permutation(jax.random.fold_in(arg_keys[1], 3), TOKENS // TOK_DEV)
    routes = jax.vmap(lambda own, number: assign_block(jax.random.fold_in(arg_keys[1], 2), own, number, TOK_DEV, EXPERTS, 2, TOK_DEV // 2, 2))(routes_keys, routes_turns).reshape((TOKENS, 2))
    w_router = gaussian(arg_keys[2], (D, EXPERTS), D ** -0.5, 0.078125)
    w_gate = gaussian(arg_keys[3], (D, EXPERTS * FF_W), D ** -0.5, 0.078125, ((1, 32),))
    w_up = gaussian(arg_keys[4], (D, EXPERTS * FF_W), D ** -0.5, 0.078125, ((1, 32),))
    w_down = heavy_noise(arg_keys[5], (EXPERTS * FF_W, D), FF_W ** -0.5, 0.125, ((0, 32),), (0, 1, 32, 2.75))
    return dict(tokens=tokens, routes=routes, w_router=w_router, w_gate=w_gate, w_up=w_up, w_down=w_down)


def pair_weights(logits, routes):
    picks = jnp.sum(jnp.where(routes[:, :, None] == jnp.arange(EXPERTS)[None, None, :], logits[:, None, :], 0.0), axis=2)
    first = 1.0 / (1.0 + jnp.exp(picks[:, 1] - picks[:, 0]))
    second = 1.0 / (1.0 + jnp.exp(picks[:, 0] - picks[:, 1]))
    return jnp.stack([first, second], axis=1)


def reference(tokens, routes, w_router, w_gate, w_up, w_down):
    logits = jnp.dot(tokens, w_router, preferred_element_type=jnp.float32)
    weights = pair_weights(logits, routes)
    repeat = max(1, N_EXPERT // EXPERTS)
    width = EXPERTS * FF_W // (N_EXPERT * N_SHARD)
    blocks = FF_W // (repeat * width)
    rows_most = N_EXPERT * (TOK_DEV // 2)
    mixed = jnp.zeros((TOKENS, D), jnp.float32)
    for expert in range(EXPERTS):
        hit = routes == expert
        coef = jnp.sum(jnp.where(hit, weights, 0.0), axis=1)
        routed = jnp.any(hit, axis=1)
        index = jnp.nonzero(routed, size=rows_most, fill_value=0)[0].astype(jnp.int32)
        valid = jnp.arange(rows_most) < jnp.sum(routed.astype(jnp.int32))
        chosen = tokens[index]
        low = expert * FF_W
        gate = jnp.dot(chosen, w_gate[:, low:low + FF_W], preferred_element_type=jnp.float32)
        up = jnp.dot(chosen, w_up[:, low:low + FF_W], preferred_element_type=jnp.float32)
        hidden = (jax.nn.silu(gate) * up).astype(jnp.bfloat16)
        hidden_blocks = hidden.reshape(rows_most, repeat * blocks, width)
        down_blocks = w_down[low:low + FF_W].reshape(repeat * blocks, width, D)
        total = jnp.zeros((rows_most, D), jnp.float32)
        for part in range(repeat):
            def add_block(step, acc):
                which = part * blocks + step
                left = lax.dynamic_index_in_dim(hidden_blocks, which, 1, keepdims=False)
                right = lax.dynamic_index_in_dim(down_blocks, which, 0, keepdims=False)
                term = jnp.dot(left, right, preferred_element_type=jnp.float32).astype(jnp.bfloat16)
                return acc + lax.optimization_barrier(term).astype(jnp.float32)
            part_sum = lax.fori_loop(0, blocks, add_block, jnp.zeros((rows_most, D), jnp.float32))
            rounded = lax.optimization_barrier(part_sum.astype(jnp.bfloat16))
            total = total + rounded.astype(jnp.float32)
        contrib = jnp.where(valid[:, None], coef[index][:, None] * total, 0.0)
        mixed = mixed.at[index].add(contrib)
    return mixed.astype(jnp.bfloat16)
```

```python
import functools
import jax
import jax.numpy as jnp
from jax import lax
from jax.experimental import pallas as pl
from jax.experimental.pallas import tpu as pltpu
from jax.sharding import PartitionSpec as P

CAP = 16
WD_SLOTS = 3
F32 = jnp.float32
BF16 = jnp.bfloat16


def _nblock(n):
    for b in (512, 384, 256, 128):
        if n % b == 0:
            return b
    return n


def kernel(cfg, tok_hbm, routes_hbm, wr_hbm, wg_hbm, wu_hbm, wd_hbm, out_ref,
           tok, routes, wr, wg, wu, wd, bucket, xin, accg, accu, hid, ps, po, pin, sb, rin,
           lpart, lin, small_sem, wg_sem, wu_sem, wd_sem, x_sem, xs_sem, l_sem, ls_sem, f_sem,
           p_sem, pss_sem, r_sem, rs_sem):
    G, S, E, T, DP, W, D = cfg
    nchip = S // 2
    rows = G * CAP
    g_me = lax.axis_index("expert")
    s_me = lax.axis_index("shard")
    core = lax.rem(s_me, 2)
    chip = s_me // 2
    partner = chip * 2 + (1 - core)
    per_chunk = 1 if DP % 128 == 0 else 2
    nchunk = S // per_chunk
    cw = per_chunk * DP

    def src_at(i):
        k, half = i // 2, lax.rem(i, 2)
        par = jnp.where(half == 0, core, 1 - core)
        return lax.rem(chip + k, nchip) * 2 + par

    def dest_chip(j):
        return lax.rem(chip + 1 + j, nchip)

    smalls = [
        pltpu.make_async_copy(tok_hbm, tok, small_sem.at[0]),
        pltpu.make_async_copy(routes_hbm, routes, small_sem.at[1]),
        pltpu.make_async_copy(wr_hbm, wr, small_sem.at[2]),
    ]
    for c in smalls:
        c.start()

    def w_copy(i):
        s = src_at(i)
        r = pl.ds(pl.multiple_of(s * DP, 16), DP)
        return (pltpu.make_async_copy(wg_hbm.at[r, :], wg.at[i], wg_sem.at[i]),
                pltpu.make_async_copy(wu_hbm.at[r, :], wu.at[i], wu_sem.at[i]))

    def start_w(i, _):
        a, b = w_copy(i)
        a.start()
        b.start()
        return 0

    lax.fori_loop(0, S, start_w, 0)

    def wd_copy(k):
        if per_chunk == 1:
            j, second = k // 2, k % 2
            par = core if second else 1 - core
            col = (dest_chip(j) * 2 + par) * DP
        else:
            col = dest_chip(k) * cw
        return pltpu.make_async_copy(
            wd_hbm.at[:, pl.ds(pl.multiple_of(col, 128), cw)], wd.at[k % WD_SLOTS], wd_sem.at[k % WD_SLOTS])

    for k in range(min(WD_SLOTS, nchunk)):
        wd_copy(k).start()

    barrier = pltpu.get_barrier_semaphore()

    def greet(d, _):
        pl.semaphore_signal(barrier, inc=1, device_id={"expert": d // S, "shard": lax.rem(d, S)},
                            device_id_type=pl.DeviceIdType.MESH)
        return 0

    def greet_core(i, _):
        q = lax.rem(g_me * nchip + chip + i, G * nchip)
        return greet(q * 2 + core, 0)

    def greet_other(i, _):
        return greet(g_me * S + i * 2 + 1 - core, 0)

    lax.fori_loop(1, G * nchip, greet_core, 0)
    lax.fori_loop(0, nchip, greet_other, 0)

    for c in smalls:
        c.wait()

    ones = lambda m: jnp.where(m, 1.0, 0.0).astype(BF16)
    io = lambda shape, d: lax.broadcasted_iota(jnp.int32, shape, d)
    sub_e = io((E * CAP, T), 0) // CAP
    sub_slot = lax.rem(io((E * CAP, T), 0), CAP)
    named = (sub_e == routes[0:1, :]) | (sub_e == routes[1:2, :])
    ahead = ones(io((T, T), 0) < io((T, T), 1))
    rank = jnp.dot(ones(named), ahead, preferred_element_type=F32)
    place = ones(named & (rank == sub_slot.astype(F32)))
    tokv = tok[...]
    got = jnp.dot(place, tokv, preferred_element_type=F32)
    bucket[...] = got.astype(BF16).reshape(E, CAP, DP)

    pl.semaphore_wait(barrier, G * nchip - 1 + nchip)

    def x_local():
        e = (g_me * S + s_me) * E // (G * S)
        return pltpu.make_async_copy(
            bucket.at[e], xin.at[s_me, pl.ds(pl.multiple_of(g_me * CAP, CAP), CAP), :], x_sem.at[s_me])

    def x_remote(i):
        k, gi = i // G, lax.rem(i, G)
        g, s = lax.rem(g_me + gi, G), lax.rem(chip - k + nchip, nchip) * 2 + core
        e = (g * S + s) * E // (G * S)
        return pltpu.make_async_remote_copy(
            src_ref=bucket.at[e], dst_ref=xin.at[s_me, pl.ds(pl.multiple_of(g_me * CAP, CAP), CAP), :],
            send_sem=xs_sem, recv_sem=x_sem.at[s_me], device_id={"expert": g, "shard": s},
            device_id_type=pl.DeviceIdType.MESH)

    x_local().start()

    def x_start(i, _):
        x_remote(i).start()
        return 0

    lax.fori_loop(1, G * nchip, x_start, 0)

    spread = ones(io((E * CAP, E), 0) // CAP == io((E * CAP, E), 1))
    for s in range(S):
        @pl.when(s_me == s)
        def _(s=s):
            piece = wr[:, s * DP:(s + 1) * DP]
            wide = jnp.dot(spread, piece, preferred_element_type=F32).astype(BF16)
            lpart[...] = lax.dot_general(tokv, wide, (((1,), (1,)), ((), ())), preferred_element_type=F32)


    def l_copy(i):
        return pltpu.make_async_remote_copy(
            src_ref=lpart, dst_ref=lin.at[s_me], send_sem=ls_sem, recv_sem=l_sem,
            device_id={"expert": g_me, "shard": lax.rem(s_me + i, S)},
            device_id_type=pl.DeviceIdType.MESH)

    def l_start(i, _):
        l_copy(i).start()
        return 0


    def forward(s):
        return pltpu.make_async_remote_copy(
            src_ref=xin.at[s], dst_ref=xin.at[s], send_sem=f_sem, recv_sem=x_sem.at[s],
            device_id={"expert": g_me, "shard": partner}, device_id_type=pl.DeviceIdType.MESH)

    accg[...] = jnp.zeros_like(accg)
    accu[...] = jnp.zeros_like(accu)
    nb = _nblock(W)

    def up_step(i, _):
        s = src_at(i)
        pltpu.make_async_copy(xin.at[s], xin.at[s], x_sem.at[s]).wait()

        @pl.when(lax.rem(i, 2) == 0)
        def _():
            forward(s).start()

        a, b = w_copy(i)
        a.wait()
        b.wait()
        x = xin[s]
        for n in range(0, W, nb):
            accg[:, n:n + nb] += jnp.dot(x, wg[i, :, n:n + nb], preferred_element_type=F32)
            accu[:, n:n + nb] += jnp.dot(x, wu[i, :, n:n + nb], preferred_element_type=F32)
        return 0

    lax.fori_loop(0, S, up_step, 0)
    lax.fori_loop(1, S, l_start, 0)

    for n in range(0, W, nb):
        gate = accg[:, n:n + nb]
        hid[:, n:n + nb] = (gate / (1.0 + jnp.exp(-gate)) * accu[:, n:n + nb]).astype(BF16)

    def down(k, store):
        wd_copy(k).wait()
        slot = k % WD_SLOTS
        h = hid[...]
        cb = 256 if cw % 256 == 0 else cw
        for n in range(0, cw, cb):
            store(n, cb, jnp.dot(h, wd[slot, :, n:n + cb], preferred_element_type=F32))
        if k + WD_SLOTS < nchunk:
            wd_copy(k + WD_SLOTS).start()

    def pair_copy(j):
        return pltpu.make_async_remote_copy(
            src_ref=ps.at[j], dst_ref=pin.at[j], send_sem=pss_sem, recv_sem=p_sem.at[j],
            device_id={"expert": g_me, "shard": partner}, device_id_type=pl.DeviceIdType.MESH)

    q_me = g_me * nchip + chip

    def home(j, gi):
        g = lax.rem(g_me + gi, G)
        dchip = dest_chip(j)
        src = sb.at[j, pl.ds(pl.multiple_of(g * CAP, CAP), CAP), :]
        dst = rin.at[pl.ds(pl.multiple_of(q_me * CAP, CAP), CAP), :]
        if j == nchip - 1 and gi == 0:
            return pltpu.make_async_copy(src, dst, r_sem)
        return pltpu.make_async_remote_copy(
            src_ref=src, dst_ref=dst, send_sem=rs_sem, recv_sem=r_sem,
            device_id={"expert": g, "shard": dchip * 2 + core}, device_id_type=pl.DeviceIdType.MESH)

    def finish(j):
        pair_copy(j).wait_recv()
        sb[j] = (po[j] + pin[j].astype(F32)).astype(BF16)
        for gi in list(range(1, G)) + [0]:
            home(j, gi).start()

    for j in range(nchip):
        if per_chunk == 1:
            def to_ps(n, cb, v, j=j):
                ps[j, :, n:n + cb] = v.astype(BF16)

            def to_po(n, cb, v, j=j):
                po[j, :, n:n + cb] = v

            down(2 * j, to_ps)
            pair_copy(j).start()
            if j >= 1:
                finish(j - 1)
            down(2 * j + 1, to_po)
        else:
            def to_both(n, cb, v, j=j):
                a, b = v[:, :DP], v[:, DP:]
                ps[j] = jnp.where(core == 0, b, a).astype(BF16)
                po[j] = jnp.where(core == 0, a, b)

            down(j, to_both)
            pair_copy(j).start()
        if j >= 1 and per_chunk != 1:
            finish(j - 1)
    finish(nchip - 1)

    Q = G * nchip
    nper = Q // E
    eye = ones(io((T, T), 0) == io((T, T), 1))
    rt = lax.dot_general(eye, routes[...].astype(F32).astype(BF16), (((1,), (1,)), ((), ())),
                         preferred_element_type=F32)
    r0, r1 = rt[:, 0:1].astype(jnp.int32), rt[:, 1:2].astype(jnp.int32)
    lane = io((T, Q * CAP), 1)
    lane_e, lane_slot = lane // CAP // nper, lax.rem(lane, CAP)
    is0, is1 = lane_e == r0, lane_e == r1
    before = ones(io((T, T), 1) < io((T, T), 0))
    rank = jnp.dot(before, ones(is0 | is1), preferred_element_type=F32)
    here = (is0 | is1) & (rank == lane_slot.astype(F32))

    pltpu.make_async_copy(lin.at[pl.ds(0, S - 1)], lin.at[pl.ds(0, S - 1)], l_sem).wait()
    lin[s_me] = lpart[...]
    logits = jnp.sum(lin[...], axis=0)
    small = io((T, E * CAP), 1)
    p0 = jnp.sum(jnp.where(small == r0 * CAP, logits, 0.0), axis=1, keepdims=True)
    p1 = jnp.sum(jnp.where(small == r1 * CAP, logits, 0.0), axis=1, keepdims=True)
    first = 1.0 / (1.0 + jnp.exp(p1 - p0))
    second = 1.0 / (1.0 + jnp.exp(p0 - p1))
    combine = jnp.where(here, jnp.where(is0, first, second), 0.0)
    high = combine.astype(BF16)
    low = (combine - high.astype(F32)).astype(BF16)

    pltpu.make_async_copy(rin, rin, r_sem).wait()
    back = rin[...]
    out_ref[...] = (jnp.dot(high, back, preferred_element_type=F32)
                    + jnp.dot(low, back, preferred_element_type=F32)).astype(BF16)

    def sent(ref, sem):
        pltpu.make_async_copy(ref, ref, sem).wait()

    sent(rin.at[pl.ds(0, (G * nchip - 1) * CAP)], xs_sem)
    sent(lin.at[pl.ds(0, S - 1)], ls_sem)
    sent(ps, f_sem)
    sent(ps, pss_sem)
    sent(rin.at[pl.ds(0, (G * nchip - 1) * CAP)], rs_sem)


def local(G, S, tokens, routes, w_router, w_gate, w_up, w_down):
    T, DP = tokens.shape
    D, E = w_router.shape
    W = w_gate.shape[1]
    nchip, rows = S // 2, G * CAP
    assert T // 2 <= CAP and S % 2 == 0 and (G * nchip) % E == 0
    cw = DP if DP % 128 == 0 else 2 * DP
    cfg = (G, S, E, T, DP, W, D)
    any_spec = pl.BlockSpec(memory_space=pl.ANY)
    dma = pltpu.SemaphoreType.DMA
    V = pltpu.VMEM
    return pl.pallas_call(
        functools.partial(kernel, cfg),
        out_shape=jax.ShapeDtypeStruct((T, DP), BF16),
        in_specs=[any_spec] * 6,
        out_specs=pl.BlockSpec(memory_space=pltpu.VMEM),
        scratch_shapes=[
            V((T, DP), BF16), V((2, T), jnp.int32), V((E, D), BF16),
            V((S, DP, W), BF16), V((S, DP, W), BF16), V((WD_SLOTS, W, cw), BF16),
            V((E, CAP, DP), BF16), V((S, rows, DP), BF16),
            V((rows, W), F32), V((rows, W), F32), V((rows, W), BF16),
            V((nchip, rows, DP), BF16), V((nchip, rows, DP), F32), V((nchip, rows, DP), BF16),
            V((nchip, rows, DP), BF16), V((G * nchip * CAP, DP), BF16),
            V((T, E * CAP), F32), V((S, T, E * CAP), F32),
            dma((3,)), dma((S,)), dma((S,)), dma((WD_SLOTS,)), dma((S,)), dma, dma, dma, dma,
            dma((nchip,)), dma, dma, dma,
        ],
        compiler_params=pltpu.CompilerParams(
            collective_id=0, has_side_effects=True, vmem_limit_bytes=67043328),
    )(tokens, routes.T, w_router.T, w_gate, w_up, w_down)


def solution(mesh):
    return jax.shard_map(
        functools.partial(local, mesh.shape["expert"], mesh.shape["shard"]),
        mesh=mesh,
        in_specs=(
            P("expert", "shard"),
            P("expert", None),
            P(),
            P(None, ("expert", "shard")),
            P(None, ("expert", "shard")),
            P(("expert", "shard"), None),
        ),
        out_specs=P("expert", "shard"),
        check_vma=False,
    )
```

```python
import functools
import jax
import jax.numpy as jnp
from jax import lax
from jax.experimental import pallas as pl
from jax.experimental.pallas import tpu as pltpu
from jax.sharding import PartitionSpec as P

CAP = 16
WD_SLOTS = 3
F32 = jnp.float32
BF16 = jnp.bfloat16


def _nblock(n):
    for b in (512, 384, 256, 128):
        if n % b == 0:
            return b
    return n


def _rows(w, dp):
    return [(r, min(dp, w - r)) for r in range(0, w, dp)]


def _shared(nchip, S, DP, W):
    return DP % 128 == 0 and 2 * DP <= W and nchip * len(_rows(W, DP)) <= 2 * (S - 2)


def kernel(cfg, tok_hbm, routes_hbm, wr_hbm, wg_hbm, wu_hbm, wd_hbm, out_ref,
           tok, routes, wr, wg, wu, wd, bucket, xin, accg, accu, hid, ps, po, pin, sb, rin,
           lpart, lin, small_sem, wg_sem, wu_sem, wd_sem, x_sem, xs_sem, l_sem, ls_sem, f_sem,
           p_sem, pss_sem, r_sem, rs_sem):
    G, S, E, T, DP, W, D = cfg
    nchip = S // 2
    rows = G * CAP
    quad = CAP // 4
    most = -(-(T // 2) // 4)
    g_me = lax.axis_index("expert")
    s_me = lax.axis_index("shard")
    core = lax.rem(s_me, 2)
    chip = s_me // 2
    partner = chip * 2 + (1 - core)
    per_chunk = 1 if DP % 128 == 0 else 2
    nchunk = S // per_chunk
    cw = per_chunk * DP

    def src_at(i):
        half = i // nchip
        return lax.rem(chip + i - half * nchip, nchip) * 2 + 1 - half

    def dest_chip(j):
        return lax.rem(chip + 1 + j, nchip)

    smalls = [
        pltpu.make_async_copy(tok_hbm, tok, small_sem.at[0]),
        pltpu.make_async_copy(routes_hbm, routes, small_sem.at[1]),
        pltpu.make_async_copy(wr_hbm, wr, small_sem.at[2]),
    ]
    for c in smalls:
        c.start()

    def w_copy(i):
        s = src_at(i)
        r = pl.ds(pl.multiple_of(s * DP, 16), DP)
        return (pltpu.make_async_copy(wg_hbm.at[r, :], wg.at[i], wg_sem.at[i]),
                pltpu.make_async_copy(wu_hbm.at[r, :], wu.at[i], wu_sem.at[i]))

    def start_w(i, _):
        a, b = w_copy(i)
        a.start()
        b.start()
        return 0

    lax.fori_loop(0, S, start_w, 0)

    def wd_copy(k):
        if per_chunk == 1:
            j, second = k // 2, k % 2
            par = core if second else 1 - core
            col = (dest_chip(j) * 2 + par) * DP
        else:
            col = dest_chip(k) * cw
        return pltpu.make_async_copy(
            wd_hbm.at[:, pl.ds(pl.multiple_of(col, 128), cw)], wd.at[k % WD_SLOTS], wd_sem.at[k % WD_SLOTS])

    shared = _shared(nchip, S, DP, W)
    blocks = _rows(W, DP)
    if not shared:
        for k in range(min(WD_SLOTS, nchunk)):
            wd_copy(k).start()

    def home_of(j, r):
        b = j * len(blocks) + r
        return (wg, wu)[b % 2], b // 2

    def block_copy(j, r, half):
        buf, slot = home_of(j, r)
        par = core if half else 1 - core
        low, high = pl.multiple_of(par * DP, 128), blocks[r][0]
        col = pl.multiple_of((dest_chip(j) * 2 + par) * DP, 128)
        return pltpu.make_async_copy(
            wd_hbm.at[pl.ds(high, blocks[r][1]), pl.ds(col, DP)],
            buf.at[slot, pl.ds(0, blocks[r][1]), pl.ds(low, DP)],
            wd_sem.at[(j * len(blocks) + r) * 2 + half])

    def refill(i):
        for b in (2 * i, 2 * i + 1):
            if b < nchip * len(blocks):
                for half in range(2):
                    block_copy(b // len(blocks), b % len(blocks), half).start()

    def blank(q, _):
        for r in range(most, quad):
            rin[q * quad + r] = jnp.zeros((4, DP), BF16)
        return 0

    lax.fori_loop(0, G * nchip, blank, 0)
    barrier = pltpu.get_barrier_semaphore()

    def greet(d, _):
        pl.semaphore_signal(barrier, inc=1, device_id={"expert": d // S, "shard": lax.rem(d, S)},
                            device_id_type=pl.DeviceIdType.MESH)
        return 0

    def greet_core(i, _):
        q = lax.rem(g_me * nchip + chip + i, G * nchip)
        return greet(q * 2 + core, 0)

    def greet_other(i, _):
        return greet(g_me * S + i * 2 + 1 - core, 0)

    lax.fori_loop(1, G * nchip, greet_core, 0)
    lax.fori_loop(0, nchip, greet_other, 0)

    for c in smalls:
        c.wait()

    ones = lambda m: jnp.where(m, 1.0, 0.0).astype(BF16)
    io = lambda shape, d: lax.broadcasted_iota(jnp.int32, shape, d)
    sub_e = io((E * CAP, T), 0) // CAP
    sub_slot = lax.rem(io((E * CAP, T), 0), CAP)
    named = (sub_e == routes[0:1, :]) | (sub_e == routes[1:2, :])
    ahead = ones(io((T, T), 0) < io((T, T), 1))
    rank = jnp.dot(ones(named), ahead, preferred_element_type=F32)
    place = ones(named & (rank == sub_slot.astype(F32)))
    tokv = tok[...]
    got = jnp.dot(place, tokv, preferred_element_type=F32)
    bucket[...] = got.reshape(E, quad, 4, DP).astype(BF16)

    pl.semaphore_wait(barrier, G * nchip - 1 + nchip)

    def x_local():
        e = (g_me * S + s_me) * E // (G * S)
        return pltpu.make_async_copy(
            bucket.at[e, pl.ds(0, most)], xin.at[s_me, pl.ds(g_me * quad, most)], x_sem.at[s_me])

    def x_remote(i):
        k, gi = i // G, lax.rem(i, G)
        g, s = lax.rem(g_me + gi, G), lax.rem(chip - k + nchip, nchip) * 2 + core
        e = (g * S + s) * E // (G * S)
        return pltpu.make_async_remote_copy(
            src_ref=bucket.at[e, pl.ds(0, most)],
            dst_ref=xin.at[s_me, pl.ds(g_me * quad, most)],
            send_sem=xs_sem, recv_sem=x_sem.at[s_me], device_id={"expert": g, "shard": s},
            device_id_type=pl.DeviceIdType.MESH)

    x_local().start()

    def x_start(i, _):
        x_remote(i).start()
        return 0

    lax.fori_loop(1, G * nchip, x_start, 0)

    spread = ones(io((E * CAP, E), 0) // CAP == io((E * CAP, E), 1))
    for s in range(S):
        @pl.when(s_me == s)
        def _(s=s):
            piece = wr[:, s * DP:(s + 1) * DP]
            wide = jnp.dot(spread, piece, preferred_element_type=F32).astype(BF16)
            lpart[...] = lax.dot_general(tokv, wide, (((1,), (1,)), ((), ())), preferred_element_type=F32)


    def l_copy(i):
        return pltpu.make_async_remote_copy(
            src_ref=lpart, dst_ref=lin.at[s_me], send_sem=ls_sem, recv_sem=l_sem,
            device_id={"expert": g_me, "shard": lax.rem(s_me + i, S)},
            device_id_type=pl.DeviceIdType.MESH)

    def l_start(i, _):
        l_copy(i).start()
        return 0


    def forward(s):
        for g in range(G):
            piece = xin.at[s, pl.ds(g * quad, most)]
            pltpu.make_async_remote_copy(
                src_ref=piece, dst_ref=piece, send_sem=f_sem, recv_sem=x_sem.at[s],
                device_id={"expert": g_me, "shard": partner}, device_id_type=pl.DeviceIdType.MESH).start()

    accg[...] = jnp.zeros_like(accg)
    accu[...] = jnp.zeros_like(accu)
    nb = _nblock(W)

    def up_step(i, _):
        s = src_at(i)

        def arrived(s):
            got = xin.at[s, pl.ds(0, G * most)]
            pltpu.make_async_copy(got, got, x_sem.at[s]).wait()

        @pl.when((core == 0) & (i >= nchip - 1) & (i < S - 1))
        def _():
            ahead = src_at(i + 1)
            arrived(ahead)
            forward(ahead)

        @pl.when((core == 1) | (i < nchip))
        def _():
            arrived(s)

        @pl.when((core == 1) & (i < nchip))
        def _():
            forward(s)

        a, b = w_copy(i)
        a.wait()
        b.wait()
        x = xin[s].reshape(rows, DP)
        for n in range(0, W, nb):
            accg[:, n:n + nb] += jnp.dot(x, wg[i, :, n:n + nb], preferred_element_type=F32)
            accu[:, n:n + nb] += jnp.dot(x, wu[i, :, n:n + nb], preferred_element_type=F32)
        return 0

    if shared:
        lax.fori_loop(0, 2, up_step, 0)
        for i in range(2, S):
            up_step(i, 0)
            refill(i - 2)
    else:
        lax.fori_loop(0, S, up_step, 0)
    lax.fori_loop(1, S, l_start, 0)

    for n in range(0, W, nb):
        gate = accg[:, n:n + nb]
        hid[:, n:n + nb] = (gate / (1.0 + jnp.exp(-gate)) * accu[:, n:n + nb]).astype(BF16)

    def down(k, store):
        wd_copy(k).wait()
        slot = k % WD_SLOTS
        h = hid[...]
        cb = 256 if cw % 256 == 0 else cw
        for n in range(0, cw, cb):
            store(n, cb, jnp.dot(h, wd[slot, :, n:n + cb], preferred_element_type=F32))
        if k + WD_SLOTS < nchunk:
            wd_copy(k + WD_SLOTS).start()

    def pair_copy(j):
        return pltpu.make_async_remote_copy(
            src_ref=ps.at[j], dst_ref=pin.at[j], send_sem=pss_sem, recv_sem=p_sem.at[j],
            device_id={"expert": g_me, "shard": partner}, device_id_type=pl.DeviceIdType.MESH)

    q_me = g_me * nchip + chip

    def home(j, gi):
        g = lax.rem(g_me + gi, G)
        dchip = dest_chip(j)
        src = sb.at[j, pl.ds(g * quad, most)]
        dst = rin.at[pl.ds(q_me * quad, most)]
        if j == nchip - 1 and gi == 0:
            return pltpu.make_async_copy(src, dst, r_sem)
        return pltpu.make_async_remote_copy(
            src_ref=src, dst_ref=dst, send_sem=rs_sem, recv_sem=r_sem,
            device_id={"expert": g, "shard": dchip * 2 + core}, device_id_type=pl.DeviceIdType.MESH)

    def finish(j):
        pair_copy(j).wait_recv()
        send_home(j)

    def send_home(j):
        sb[j] = (po[j] + pin[j].astype(F32)).reshape(G * quad, 4, DP).astype(BF16)
        for gi in list(range(1, G)) + [0]:
            home(j, gi).start()

    cb = 256 if DP % 256 == 0 else 128
    tiles = [(half, n) for half in range(2) for n in range(0, DP, cb)]
    early = DP // cb + DP // cb % 2

    def columns(j, todo):
        for half, n in todo:
            par = core if half else 1 - core
            tot = None
            for r, (high, depth) in enumerate(blocks):
                buf, slot = home_of(j, r)
                one = jnp.dot(hid[:, high:high + depth],
                              buf[slot, 0:depth, pl.ds(pl.multiple_of(par * DP + n, 128), cb)],
                              preferred_element_type=F32)
                tot = one if tot is None else tot + one
            if half:
                po[j, :, n:n + cb] = tot
            else:
                ps[j, :, n:n + cb] = tot.astype(BF16)

    def landed(j, half):
        for r in range(len(blocks)):
            block_copy(j, r, half).wait()

    for j in range(nchip):
        if per_chunk == 1:
            def to_ps(n, cb, v, j=j):
                ps[j, :, n:n + cb] = v.astype(BF16)

            def to_po(n, cb, v, j=j):
                po[j, :, n:n + cb] = v

            if shared:
                if j == 0:
                    landed(0, 0)
                    landed(0, 1)
                last = j == nchip - 1
                first = len(tiles) // 2 if last else early
                if last and j > 0:
                    landed(j, 0)
                columns(j, tiles[:first])
                pair_copy(j).start()
                if j >= 1:
                    pair_copy(j - 1).wait_recv()
                    send_home(j - 1)
                if j < nchip - 2:
                    landed(j + 1, 0)
                    landed(j + 1, 1)
                if last and j > 0:
                    landed(j, 1)
                columns(j, tiles[first:])
            else:
                down(2 * j, to_ps)
                pair_copy(j).start()
                if j >= 1:
                    finish(j - 1)
                down(2 * j + 1, to_po)
        else:
            def to_both(n, cb, v, j=j):
                a, b = v[:, :DP], v[:, DP:]
                ps[j] = jnp.where(core == 0, b, a).astype(BF16)
                po[j] = jnp.where(core == 0, a, b)

            down(j, to_both)
            pair_copy(j).start()
            if j >= 1:
                finish(j - 1)
    finish(nchip - 1)

    Q = G * nchip
    nper = Q // E
    eye = ones(io((T, T), 0) == io((T, T), 1))
    rt = lax.dot_general(eye, routes[...].astype(F32).astype(BF16), (((1,), (1,)), ((), ())),
                         preferred_element_type=F32)
    r0, r1 = rt[:, 0:1].astype(jnp.int32), rt[:, 1:2].astype(jnp.int32)
    lane = io((T, Q * CAP), 1)
    lane_e, lane_slot = lane // CAP // nper, lax.rem(lane, CAP)
    is0, is1 = lane_e == r0, lane_e == r1
    before = ones(io((T, T), 1) < io((T, T), 0))
    rank = jnp.dot(before, ones(is0 | is1), preferred_element_type=F32)
    here = (is0 | is1) & (rank == lane_slot.astype(F32))

    pltpu.make_async_copy(lin.at[pl.ds(0, S - 1)], lin.at[pl.ds(0, S - 1)], l_sem).wait()
    lin[s_me] = lpart[...]
    logits = jnp.sum(lin[...], axis=0)
    small = io((T, E * CAP), 1)
    p0 = jnp.sum(jnp.where(small == r0 * CAP, logits, 0.0), axis=1, keepdims=True)
    p1 = jnp.sum(jnp.where(small == r1 * CAP, logits, 0.0), axis=1, keepdims=True)
    first = 1.0 / (1.0 + jnp.exp(p1 - p0))
    second = 1.0 / (1.0 + jnp.exp(p0 - p1))
    combine = jnp.where(here, jnp.where(is0, first, second), 0.0)
    high = combine.astype(BF16)
    low = (combine - high.astype(F32)).astype(BF16)

    got = rin.at[pl.ds(0, Q * most)]
    pltpu.make_async_copy(got, got, r_sem).wait()
    back = rin[...].reshape(Q * CAP, DP)
    out_ref[...] = (jnp.dot(high, back, preferred_element_type=F32)
                    + jnp.dot(low, back, preferred_element_type=F32)).astype(BF16)

    def sent(ref, sem):
        pltpu.make_async_copy(ref, ref, sem).wait()

    sent(rin.at[pl.ds(0, (Q - 1) * most)], xs_sem)
    sent(lin.at[pl.ds(0, S - 1)], ls_sem)
    sent(xin.at[pl.ds(0, nchip), pl.ds(0, G * most)], f_sem)
    sent(ps, pss_sem)
    sent(rin.at[pl.ds(0, (Q - 1) * most)], rs_sem)


def local(G, S, tokens, routes, w_router, w_gate, w_up, w_down):
    T, DP = tokens.shape
    D, E = w_router.shape
    W = w_gate.shape[1]
    nchip, rows = S // 2, G * CAP
    assert T // 2 <= CAP and S % 2 == 0 and (G * nchip) % E == 0
    cw = DP if DP % 128 == 0 else 2 * DP
    shared = _shared(nchip, S, DP, W)
    nwd = 2 * nchip * len(_rows(W, DP)) if shared else WD_SLOTS
    cfg = (G, S, E, T, DP, W, D)
    any_spec = pl.BlockSpec(memory_space=pl.ANY)
    dma = pltpu.SemaphoreType.DMA
    V = pltpu.VMEM
    return pl.pallas_call(
        functools.partial(kernel, cfg),
        out_shape=V((T, DP), BF16),
        in_specs=[any_spec] * 6,
        out_specs=pl.BlockSpec(memory_space=pltpu.VMEM),
        scratch_shapes=[
            V((T, DP), BF16), V((2, T), jnp.int32), V((E, D), BF16),
            V((S, DP, W), BF16), V((S, DP, W), BF16), V((1, 16, 128) if shared else (WD_SLOTS, W, cw), BF16),
            V((E, CAP // 4, 4, DP), BF16), V((S, rows // 4, 4, DP), BF16),
            V((rows, W), F32), V((rows, W), F32), V((rows, W), BF16),
            V((nchip, rows, DP), BF16), V((nchip, rows, DP), F32), V((nchip, rows, DP), BF16),
            V((nchip, rows // 4, 4, DP), BF16), V((G * nchip * CAP // 4, 4, DP), BF16),
            V((T, E * CAP), F32), V((S, T, E * CAP), F32),
            dma((3,)), dma((S,)), dma((S,)), dma((nwd,)), dma((S,)), dma, dma, dma, dma,
            dma((nchip,)), dma, dma, dma,
        ],
        compiler_params=pltpu.CompilerParams(
            collective_id=0, has_side_effects=True, vmem_limit_bytes=63 * 1024 * 1024),
    )(tokens, routes.T, w_router.T, w_gate, w_up, w_down)


def solution(mesh):
    return jax.shard_map(
        functools.partial(local, mesh.shape["expert"], mesh.shape["shard"]),
        mesh=mesh,
        in_specs=(
            P("expert", "shard"),
            P("expert", None),
            P(),
            P(None, ("expert", "shard")),
            P(None, ("expert", "shard")),
            P(("expert", "shard"), None),
        ),
        out_specs=P("expert", "shard"),
        check_vma=False,
    )
```
